32 devices in a mesh: dp: 8 (over y, x, core), mp: 4 (over z).
Axes of the slice: x: 2, y: 2, z: 4, core: 2. Of those that a mesh axis runs over, the one named last changes fastest.
Arguments:
- tokens: bfloat16 [4096, 1024], P('dp', 'mp'), may hold values from -150 to 150
- pre_gain: bfloat16 [1024], P('mp'), may hold values from 0.25 to 1.75
- input_weight: bfloat16 [3, 1024, 1024], P(None, 'dp', 'mp'), may hold values from -0.125 to 0.125
- output_weight: bfloat16 [1024, 1024], P('mp', 'dp'), may hold values from -1 to 1
- position_bias: bfloat16 [16, 512, 512], P('mp'), may hold values from -3 to 353
- post_gain: bfloat16 [1024], P('mp'), may hold values from 0.25 to 1.75
Outputs:
- stream: bfloat16 [4096, 1024], P('dp', 'mp')
- normed: bfloat16 [4096, 1024], P('dp', 'mp')
The draws below stay inside these ranges and needn't reach their ends.
All inputs are finite; a program needn't handle non-finite values.
Results may differ from the reference program's by a relative error of at most 0.013.
Values may be sent and summed in bfloat16 or wider, within the bound.
No kernel may reach another device: no remote copies, remote signals or barrier semaphores. Data moves between devices by JAX's collectives and lax.ppermute only.
A program may use at most 64 MiB of HBM per device.

```python
import math
import jax
import jax.numpy as jnp
from jax import lax

SEQ = 512
HEAD_DIM = 64
HEADS = 16
D = 1024
INNER = 1024
TOKENS = 4096


def draw_tokens(key, part):
    subkeys = jax.random.split(jax.random.fold_in(key, 11), 4)
    column_place = jnp.arange(D, dtype=jnp.float32) / D
    baseline = jnp.clip(jax.random.normal(subkeys[0], (TOKENS, D), jnp.float32), -4.0, 4.0)
    row_scale = jnp.exp(jax.random.uniform(subkeys[2], (TOKENS, 1), jnp.float32, math.log(0.4), math.log(4.0)))
    column_scale = jnp.exp(column_place * math.log(3.0))[None, :] * jnp.exp(jax.random.uniform(subkeys[3], (1, D), jnp.float32, math.log(0.7), math.log(1.4)))
    return (baseline * row_scale * column_scale).astype(jnp.bfloat16)


def draw_position_bias(key, part):
    subkeys = jax.random.split(jax.random.fold_in(key, 23), 1)
    bias_shape = (HEADS, SEQ, SEQ)
    return jnp.clip(jax.random.normal(subkeys[0], bias_shape, jnp.float32), -3.0, 3.0).astype(jnp.bfloat16)


def raised(drawn, stream_key, source, target, blocks, factor):
    owner, partner = [(jnp.arange(drawn.shape[axis_at]) // (drawn.shape[axis_at] // blocks)).reshape([-1 if axis == axis_at else 1 for axis in range(drawn.ndim)]) for axis_at in (source, target)]
    chosen = jax.random.permutation(stream_key, blocks)[partner]
    strong = (owner == chosen) | (owner == (partner + blocks // 2) % blocks)
    return jnp.where(strong, factor * drawn, drawn)


def block_levels(rng, dims, cuts, smallest, top_value):
    factor_of, own = 1.0, jax.random.fold_in(rng, 6)
    for dim, shards_of in cuts:
        steps = jnp.exp(jax.random.uniform(jax.random.fold_in(own, dim), (shards_of,), jnp.float32, smallest / len(cuts), top_value / len(cuts)))
        factor_of = factor_of * jnp.repeat(steps, dims[dim] // shards_of).reshape([-1 if axis == dim else 1 for axis in range(len(dims))])
    return factor_of


def normal_values(key, shape, width, reach, cuts=(), kind=jnp.bfloat16):
    entries = jax.random.normal(key, shape, jnp.float32) * width
    if len(cuts) > 0:
        entries = block_levels(key, shape, cuts, -0.22, 0.18) * entries
    return jnp.clip(entries, min=-reach, max=reach).astype(kind)


def heavy_noise(stream_key, shape, width, bound, cuts, heavy, kind=jnp.bfloat16):
    array = width * jax.random.normal(stream_key, shape, jnp.float32)
    if cuts:
        array = array * block_levels(stream_key, shape, cuts, -0.22, 0.18)
    return jnp.clip(raised(array, jax.random.fold_in(stream_key, 3), *heavy), -bound, bound).astype(kind)


def setup_inputs(seed: int = 0) -> dict:
    streams_of = jax.random.split(jax.random.key(seed), 7)
    return {
        "tokens": draw_tokens(jax.random.fold_in(streams_of[6], 71), 0),
        "pre_gain": jnp.clip(1.0 + 0.15 * jax.random.normal(streams_of[1], (D,), jnp.float32), 0.25, 1.75).astype(jnp.bfloat16),
        "input_weight": normal_values(streams_of[2], (3, D, INNER), (2 * D) ** -0.5, 0.125, ((1, 8), (2, 4))),
        "output_weight": heavy_noise(streams_of[3], (INNER, D), (INNER // 16) ** -0.5, 1.0, ((0, 4), (1, 8)), (0, 1, 8, 2.0)),
        "position_bias": draw_position_bias(jax.random.fold_in(streams_of[6], 71), 0),
        "post_gain": jnp.clip(1.0 + 0.15 * jax.random.normal(streams_of[5], (D,), jnp.float32), 0.25, 1.75).astype(jnp.bfloat16),
    }


epsilon = 1e-06

def reference(tokens, pre_gain, input_weight, output_weight, position_bias, post_gain):
    widened = tokens.astype(jnp.float32)
    inverse_rms = lax.rsqrt(lax.optimization_barrier(jnp.mean(widened * widened, axis=1, keepdims=True)) + epsilon)
    normed_in = (widened * inverse_rms * pre_gain.astype(jnp.float32)).astype(jnp.bfloat16)
    projected = [jnp.dot(normed_in, input_weight[member], preferred_element_type=jnp.float32).astype(jnp.bfloat16) for member in range(3)]
    row_count = tokens.shape[0]
    bias_wide = position_bias.astype(jnp.float32)

    def one_sequence(sequence):
        offset = (sequence * SEQ).astype(jnp.int32)
        sliced = [lax.dynamic_slice_in_dim(matrix, offset, SEQ, 0).reshape(SEQ, HEADS, HEAD_DIM).astype(jnp.float32) for matrix in projected]
        scores = jnp.einsum('qhd,khd->hqk', sliced[0], sliced[1]) + bias_wide
        row_max = lax.optimization_barrier(jnp.max(scores, axis=2, keepdims=True))
        weights = jnp.exp(scores - row_max)
        probabilities = (weights / lax.optimization_barrier(jnp.sum(weights, axis=2, keepdims=True))).astype(jnp.bfloat16)
        context = jnp.einsum('hqk,khd->qhd', probabilities.astype(jnp.float32), sliced[2])
        return context.reshape(SEQ, HEADS * HEAD_DIM).astype(jnp.bfloat16)
    stacked = lax.map(one_sequence, jnp.arange(row_count // SEQ, dtype=jnp.int32))
    context = stacked.reshape(row_count, HEADS * HEAD_DIM)
    attention_out = jnp.dot(context, output_weight, preferred_element_type=jnp.float32)
    stream = (widened + attention_out).astype(jnp.bfloat16)
    restored = lax.optimization_barrier(stream).astype(jnp.float32)
    post_rms = lax.rsqrt(lax.optimization_barrier(jnp.mean(restored * restored, axis=1, keepdims=True)) + epsilon)
    normed = (restored * post_rms * post_gain.astype(jnp.float32)).astype(jnp.bfloat16)
    return (stream, normed)
```

```python
import jax
import jax.numpy as jnp
from jax import lax
from jax.experimental import pallas as pl
from jax.experimental.pallas import tpu as pltpu
from jax.sharding import PartitionSpec as P

epsilon = 1e-06


def attend_all(mixed_heads, position_bias):
    row_count = mixed_heads.shape[1]
    inner_width = mixed_heads.shape[2]
    head_count = position_bias.shape[0]
    seq_len = position_bias.shape[1]
    grouped = mixed_heads.reshape(
        3, row_count // seq_len, seq_len, head_count, inner_width // head_count
    )
    bias_wide = position_bias.astype(jnp.float32)

    def one_sequence(sequence):
        sequence_block = lax.dynamic_index_in_dim(grouped, sequence, 1, keepdims=False)
        scores = (
            jnp.einsum(
                "qhd,khd->hqk",
                sequence_block[0],
                sequence_block[1],
                preferred_element_type=jnp.float32,
            )
            + bias_wide
        )
        row_max = jnp.max(scores, axis=2, keepdims=True)
        weights = jnp.exp(scores - row_max)
        probabilities = (weights / jnp.sum(weights, axis=2, keepdims=True)).astype(jnp.bfloat16)
        context = jnp.einsum(
            "hqk,khd->qhd", probabilities, sequence_block[2], preferred_element_type=jnp.float32
        )
        return context.reshape(seq_len, inner_width).astype(jnp.bfloat16)

    stacked = lax.map(one_sequence, jnp.arange(row_count // seq_len, dtype=jnp.int32))
    return stacked.reshape(row_count, inner_width)


def on_device(tokens, pre_gain, input_weight, output_weight, position_bias, post_gain):
    rows_all, gain_all = (
        lax.all_gather(tokens, "mp", axis=1, tiled=True),
        lax.all_gather(pre_gain, "mp", axis=0, tiled=True),
    )
    widened = rows_all.astype(jnp.float32)
    inverse_rms = lax.rsqrt(jnp.mean(widened * widened, axis=1, keepdims=True) + epsilon)
    normed_in = (widened * inverse_rms * gain_all.astype(jnp.float32)).astype(jnp.bfloat16)
    feature_count = tokens.shape[1]
    projected = jnp.einsum(
        "td,kdi->kti",
        normed_in,
        lax.all_gather(input_weight, "dp", axis=1, tiled=True),
        preferred_element_type=jnp.float32,
    )
    context = attend_all(projected.astype(jnp.bfloat16), position_bias)
    partial_value = jnp.dot(
        context,
        lax.all_gather(output_weight, "dp", axis=1, tiled=True),
        preferred_element_type=jnp.float32,
    )
    attention_out = lax.psum_scatter(
        partial_value.astype(jnp.bfloat16), "mp", scatter_dimension=1, tiled=True
    ).astype(jnp.float32)
    stream = (tokens.astype(jnp.float32) + attention_out).astype(jnp.bfloat16)
    restored = lax.optimization_barrier(stream).astype(jnp.float32)
    squares = lax.psum(jnp.sum(restored * restored, axis=1), "mp")
    post_rms = lax.rsqrt(squares[:, None] / (feature_count * lax.axis_size("mp")) + epsilon)
    normed = (restored * post_rms * post_gain.astype(jnp.float32)).astype(jnp.bfloat16)
    return (stream, normed)


gain_rows = 16
lane_width = 128


def vmem_specs(count):
    return [pl.BlockSpec(memory_space=pltpu.VMEM)] * count


def attend_kernel(mp_size, dp_size, *refs):
    token_refs = refs[:mp_size]
    weight_refs = refs[mp_size : mp_size + dp_size]
    bias_ref, context_ref, normed_ref, weight_ref = refs[mp_size + dp_size :]
    seq_len, width = context_ref.shape
    head_count = bias_ref.shape[0]
    head_dim = width // head_count
    mp_at, dp_at = lax.axis_index("mp"), lax.axis_index("dp")
    rows = weight_refs[0].shape[1]
    for flip in range(dp_size):
        at = pl.multiple_of((dp_at ^ flip) * rows, rows)
        for member in range(3):
            weight_ref[member, pl.ds(at, rows), :] = weight_refs[flip][member]
    squares = jnp.zeros((seq_len, 1), jnp.float32)
    for ref in token_refs:
        part = ref[:seq_len, :].astype(jnp.float32)
        squares = squares + jnp.sum(part * part, axis=1, keepdims=True)
    features = width * mp_size
    inverse_rms = lax.rsqrt(squares / features + epsilon)
    for shift, ref in enumerate(token_refs):
        gain = ref[seq_len : seq_len + 1, :].astype(jnp.float32)
        part = ref[:seq_len, :].astype(jnp.float32)
        normed_ref[shift] = (part * inverse_rms * gain).astype(jnp.bfloat16)
    projected = []
    for member in range(3):
        total = jnp.zeros((seq_len, width), jnp.float32)
        for shift in range(mp_size):
            source = lax.rem(mp_at + (mp_size - shift), mp_size)
            at = pl.multiple_of(source * width, width)
            total = total + jnp.dot(
                normed_ref[shift],
                weight_ref[member, pl.ds(at, width), :],
                preferred_element_type=jnp.float32,
            )
        projected.append(total.astype(jnp.bfloat16))
    query, key, value = projected
    ones = jnp.ones((seq_len, head_dim), jnp.bfloat16)
    contexts = []
    for head in range(head_count):
        span = slice(head * head_dim, (head + 1) * head_dim)
        scores = lax.dot_general(
            query[:, span],
            key[:, span],
            (((1,), (1,)), ((), ())),
            preferred_element_type=jnp.float32,
        ) + bias_ref[head].astype(jnp.float32)
        row_max = jnp.max(scores, axis=1, keepdims=True)
        weights = jnp.exp(scores - row_max).astype(jnp.bfloat16)
        summed = jnp.dot(
            weights,
            jnp.concatenate([value[:, span], ones], axis=1),
            preferred_element_type=jnp.float32,
        )
        contexts.append(summed[:, :head_dim] / summed[:, head_dim : head_dim + 1])
    context_ref[...] = jnp.concatenate(contexts, axis=1).astype(jnp.bfloat16)


def finish_kernel(mp_size, dp_size, *refs):
    context_refs = refs[:mp_size]
    token_refs = refs[mp_size : 2 * mp_size]
    weight_refs = refs[2 * mp_size : 2 * mp_size + dp_size]
    gain_ref, stream_ref, normed_ref, wide_ref = refs[2 * mp_size + dp_size :]
    seq_len, width = stream_ref.shape
    mp_at, dp_at = lax.axis_index("mp"), lax.axis_index("dp")
    columns = weight_refs[0].shape[2]
    pieces = width // columns
    for shift, ref in enumerate(token_refs):
        source = lax.rem(mp_at + (mp_size - shift), mp_size)
        for piece in range(pieces):
            span = slice(piece * columns, (piece + 1) * columns)
            wide_ref[source * pieces + piece] = ref[:seq_len, span]
    squares = jnp.zeros((seq_len, columns), jnp.float32)
    for flip in range(0, dp_size, 2):
        total = jnp.zeros((seq_len, 2 * columns), jnp.float32)
        for shift in range(mp_size):
            pair = jnp.concatenate(
                [weight_refs[flip][shift], weight_refs[flip + 1][shift]], axis=1
            )
            total = total + jnp.dot(
                context_refs[shift][...], pair, preferred_element_type=jnp.float32
            )
        for half in range(2):
            at = dp_at ^ (flip + half)
            added = total[:, half * columns : (half + 1) * columns]
            stream = (wide_ref[at].astype(jnp.float32) + added).astype(jnp.bfloat16)
            wide_ref[at] = stream
            restored = stream.astype(jnp.float32)
            squares = squares + restored * restored
    mean = jnp.sum(squares, axis=1, keepdims=True) / (width * mp_size)
    post_rms = lax.rsqrt(mean + epsilon)
    for piece in range(pieces):
        span = slice(piece * columns, (piece + 1) * columns)
        stream = wide_ref[mp_at * pieces + piece]
        stream_ref[:, span] = stream
        gain = gain_ref[:, span].astype(jnp.float32)
        normed_ref[:, span] = (stream.astype(jnp.float32) * post_rms * gain).astype(jnp.bfloat16)


def from_shifts(part, size):
    return [part] + [
        lax.ppermute(part, "mp", [(at, (at + shift) % size) for at in range(size)])
        for shift in range(1, size)
    ]


def flipped(part, flip, size):
    return lax.ppermute(part, "dp", [(at, at ^ flip) for at in range(size)])


def from_flips(part, size):
    near = [part] + [flipped(part, flip, size) for flip in range(2, size, 2)]
    far = [flipped(piece, 1, size) for piece in near]
    return [piece for pair in zip(near, far) for piece in pair]


def on_device_direct(tokens, pre_gain, input_weight, output_weight, position_bias, post_gain):
    mp_size, dp_size = lax.axis_size("mp"), lax.axis_size("dp")
    seq_len, width = tokens.shape
    features = width * mp_size
    gain_block = jnp.broadcast_to(pre_gain[None, :], (gain_rows, width))
    token_parts = from_shifts(jnp.concatenate([tokens, gain_block], axis=0), mp_size)
    weight_parts = from_flips(input_weight, dp_size)
    token_parts, output_weight = lax.optimization_barrier((token_parts, output_weight))
    output_parts = from_shifts(output_weight, mp_size)
    params = pltpu.CompilerParams(vmem_limit_bytes=48 * 1024 * 1024)
    context = pl.pallas_call(
        lambda *refs: attend_kernel(mp_size, dp_size, *refs),
        out_shape=jax.ShapeDtypeStruct((seq_len, width), jnp.bfloat16),
        in_specs=vmem_specs(mp_size + dp_size + 1),
        out_specs=pl.BlockSpec(memory_space=pltpu.VMEM),
        scratch_shapes=[
            pltpu.VMEM((mp_size, seq_len, width), jnp.bfloat16),
            pltpu.VMEM((3, features, width), jnp.bfloat16),
        ],
        compiler_params=params,
        cost_estimate=pl.CostEstimate(
            flops=8 * 10**9, bytes_accessed=6 * 10**6, transcendentals=10**6
        ),
        name="attend",
    )(*token_parts, *weight_parts, position_bias)
    context, output_parts = lax.optimization_barrier((context, output_parts))
    context_parts = from_shifts(context, mp_size)
    output_all = from_flips(jnp.stack(output_parts), dp_size)
    whole = jax.ShapeDtypeStruct((seq_len, width), jnp.bfloat16)
    columns = output_weight.shape[1]
    return tuple(
        pl.pallas_call(
            lambda *refs: finish_kernel(mp_size, dp_size, *refs),
            out_shape=(whole, whole),
            in_specs=vmem_specs(2 * mp_size + dp_size + 1),
            out_specs=tuple(vmem_specs(2)),
            scratch_shapes=[pltpu.VMEM((features // columns, seq_len, columns), jnp.bfloat16)],
            compiler_params=params,
            name="finish",
        )(*context_parts, *token_parts, *output_all, post_gain[None, :])
    )


def direct_fits(mesh):
    dp_size, mp_size = mesh.shape["dp"], mesh.shape["mp"]
    return 2 <= dp_size <= 8 and dp_size & (dp_size - 1) == 0 and mp_size <= 4


def body(mesh):
    def chosen(*arrays):
        tokens, output_weight, position_bias = arrays[0], arrays[3], arrays[4]
        whole_sequence = tokens.shape[0] == position_bias.shape[1]
        lanes_fit = output_weight.shape[1] % lane_width == 0
        same_width = output_weight.shape[0] == tokens.shape[1]
        if direct_fits(mesh) and whole_sequence and lanes_fit and same_width:
            return on_device_direct(*arrays)
        return on_device(*arrays)

    return chosen


def solution(mesh):
    return jax.shard_map(
        body(mesh),
        mesh=mesh,
        in_specs=(
            P("dp", "mp"),
            P("mp"),
            P(None, "dp", "mp"),
            P("mp", "dp"),
            P("mp", None, None),
            P("mp"),
        ),
        out_specs=(P("dp", "mp"), P("dp", "mp")),
        check_vma=False,
    )
```

```python
import jax
import jax.numpy as jnp
from jax import lax
from jax.experimental import pallas as pl
from jax.experimental.pallas import tpu as pltpu
from jax.sharding import PartitionSpec as P

epsilon = 1e-06


def attend_all(mixed_heads, position_bias):
    row_count = mixed_heads.shape[1]
    inner_width = mixed_heads.shape[2]
    head_count = position_bias.shape[0]
    seq_len = position_bias.shape[1]
    grouped = mixed_heads.reshape(
        3, row_count // seq_len, seq_len, head_count, inner_width // head_count
    )
    bias_wide = position_bias.astype(jnp.float32)

    def one_sequence(sequence):
        sequence_block = lax.dynamic_index_in_dim(grouped, sequence, 1, keepdims=False)
        scores = (
            jnp.einsum(
                "qhd,khd->hqk",
                sequence_block[0],
                sequence_block[1],
                preferred_element_type=jnp.float32,
            )
            + bias_wide
        )
        row_max = jnp.max(scores, axis=2, keepdims=True)
        weights = jnp.exp(scores - row_max)
        probabilities = (weights / jnp.sum(weights, axis=2, keepdims=True)).astype(jnp.bfloat16)
        context = jnp.einsum(
            "hqk,khd->qhd", probabilities, sequence_block[2], preferred_element_type=jnp.float32
        )
        return context.reshape(seq_len, inner_width).astype(jnp.bfloat16)

    stacked = lax.map(one_sequence, jnp.arange(row_count // seq_len, dtype=jnp.int32))
    return stacked.reshape(row_count, inner_width)


def on_device(tokens, pre_gain, input_weight, output_weight, position_bias, post_gain):
    rows_all, gain_all = (
        lax.all_gather(tokens, "mp", axis=1, tiled=True),
        lax.all_gather(pre_gain, "mp", axis=0, tiled=True),
    )
    widened = rows_all.astype(jnp.float32)
    inverse_rms = lax.rsqrt(jnp.mean(widened * widened, axis=1, keepdims=True) + epsilon)
    normed_in = (widened * inverse_rms * gain_all.astype(jnp.float32)).astype(jnp.bfloat16)
    feature_count = tokens.shape[1]
    projected = jnp.einsum(
        "td,kdi->kti",
        normed_in,
        lax.all_gather(input_weight, "dp", axis=1, tiled=True),
        preferred_element_type=jnp.float32,
    )
    context = attend_all(projected.astype(jnp.bfloat16), position_bias)
    partial_value = jnp.dot(
        context,
        lax.all_gather(output_weight, "dp", axis=1, tiled=True),
        preferred_element_type=jnp.float32,
    )
    attention_out = lax.psum_scatter(
        partial_value.astype(jnp.bfloat16), "mp", scatter_dimension=1, tiled=True
    ).astype(jnp.float32)
    stream = (tokens.astype(jnp.float32) + attention_out).astype(jnp.bfloat16)
    restored = lax.optimization_barrier(stream).astype(jnp.float32)
    squares = lax.psum(jnp.sum(restored * restored, axis=1), "mp")
    post_rms = lax.rsqrt(squares[:, None] / (feature_count * lax.axis_size("mp")) + epsilon)
    normed = (restored * post_rms * post_gain.astype(jnp.float32)).astype(jnp.bfloat16)
    return (stream, normed)


lane_width = 128


def vmem_specs(count):
    return [pl.BlockSpec(memory_space=pltpu.VMEM)] * count


def prepare_kernel(mp_size, dp_size, *refs):
    weight_refs = refs[:dp_size]
    tokens_ref, bias_ref, weight_ref, tokens_out, bias_out = refs[dp_size:]
    width = tokens_ref.shape[1]
    mp_at, dp_at = lax.axis_index("mp"), lax.axis_index("dp")
    rows = weight_refs[0].shape[1]
    blocks = width // rows
    for flip in range(dp_size):
        block = dp_at ^ flip
        shift = lax.rem(mp_at + mp_size - lax.div(block, blocks), mp_size)
        at = pl.multiple_of((shift * blocks + lax.rem(block, blocks)) * rows, rows)
        for member in range(3):
            span = slice(member * width, (member + 1) * width)
            weight_ref[pl.ds(at, rows), span] = weight_refs[flip][member]
    tokens_out[...] = tokens_ref[...]
    bias_out[...] = bias_ref[...]


def attend_kernel(mp_size, *refs):
    token_refs, gain_refs = refs[:mp_size], refs[mp_size : 2 * mp_size]
    weight_ref, bias_ref, context_ref, normed_ref = refs[2 * mp_size :]
    seq_len, width = context_ref.shape
    head_count = bias_ref.shape[0]
    head_dim = width // head_count

    def lanes(member):
        return slice(member * width, (member + 1) * width)

    squares = jnp.zeros((seq_len, width), jnp.float32)
    for ref in token_refs:
        part = ref[...].astype(jnp.float32)
        squares = squares + part * part
    mean = jnp.sum(squares, axis=1, keepdims=True) / (width * mp_size)
    inverse_rms = lax.rsqrt(mean + epsilon)
    for shift, ref in enumerate(token_refs):
        gain = gain_refs[shift][...].astype(jnp.float32)
        part = ref[...].astype(jnp.float32)
        normed_ref[:, lanes(shift)] = (part * inverse_rms * gain).astype(jnp.bfloat16)
    query, key, value = [
        jnp.dot(
            normed_ref[...], weight_ref[:, lanes(member)], preferred_element_type=jnp.float32
        ).astype(jnp.bfloat16)
        for member in range(3)
    ]
    ones = jnp.ones((seq_len, head_dim), jnp.bfloat16)
    contexts = []
    for head in range(head_count):
        span = slice(head * head_dim, (head + 1) * head_dim)
        scores = lax.dot_general(
            query[:, span],
            key[:, span],
            (((1,), (1,)), ((), ())),
            preferred_element_type=jnp.float32,
        )
        scores = scores + bias_ref[head].astype(jnp.float32)
        row_max = jnp.max(scores, axis=1, keepdims=True)
        weights = jnp.exp(scores - row_max).astype(jnp.bfloat16)
        summed = jnp.dot(
            weights,
            jnp.concatenate([value[:, span], ones], axis=1),
            preferred_element_type=jnp.float32,
        )
        contexts.append(summed[:, :head_dim] / summed[:, head_dim : head_dim + 1])
    context_ref[...] = jnp.concatenate(contexts, axis=1).astype(jnp.bfloat16)


def finish_kernel(mp_size, dp_size, *refs):
    context_refs = refs[:mp_size]
    token_refs = refs[mp_size : 2 * mp_size]
    weight_refs = refs[2 * mp_size : 2 * mp_size + dp_size]
    gain_ref, stream_ref, normed_ref, wide_ref = refs[2 * mp_size + dp_size :]
    seq_len, width = stream_ref.shape
    mp_at, dp_at = lax.axis_index("mp"), lax.axis_index("dp")
    columns = weight_refs[0].shape[2]
    pieces = width // columns
    for shift, ref in enumerate(token_refs):
        source = lax.rem(mp_at + (mp_size - shift), mp_size)
        for piece in range(pieces):
            span = slice(piece * columns, (piece + 1) * columns)
            wide_ref[source * pieces + piece] = ref[:, span]
    squares = jnp.zeros((seq_len, columns), jnp.float32)
    context = jnp.concatenate([ref[...] for ref in context_refs], axis=1)
    features = width * mp_size
    for flip in range(0, dp_size, 2):
        pair = jnp.concatenate(
            [ref[...].reshape(features, columns) for ref in weight_refs[flip : flip + 2]], axis=1
        )
        total = jnp.dot(context, pair, preferred_element_type=jnp.float32)
        for half in range(2):
            at = dp_at ^ (flip + half)
            added = total[:, half * columns : (half + 1) * columns]
            stream = (wide_ref[at].astype(jnp.float32) + added).astype(jnp.bfloat16)
            wide_ref[at] = stream
            restored = stream.astype(jnp.float32)
            squares = squares + restored * restored
    mean = jnp.sum(squares, axis=1, keepdims=True) / (features)
    post_rms = lax.rsqrt(mean + epsilon)
    for piece in range(pieces):
        span = slice(piece * columns, (piece + 1) * columns)
        stream = wide_ref[mp_at * pieces + piece]
        stream_ref[:, span] = stream
        gain = gain_ref[:, span].astype(jnp.float32)
        normed_ref[:, span] = (stream.astype(jnp.float32) * post_rms * gain).astype(jnp.bfloat16)


def from_shifts(part, size):
    parts = {0: part}
    for shift in sorted(range(1, size), key=lambda shift: -min(shift, size - shift)):
        pairs = [(at, (at + shift) % size) for at in range(size)]
        parts[shift] = lax.ppermute(part, "mp", pairs)
    return [parts[shift] for shift in range(size)]


def flipped(part, flip, size):
    return lax.ppermute(part, "dp", [(at, at ^ flip) for at in range(size)])


def from_flips(part, size):
    near = [part] + [flipped(part, flip, size) for flip in range(2, size, 2)]
    far = [flipped(piece, 1, size) for piece in near]
    return [piece for pair in zip(near, far) for piece in pair]


def on_device_direct(tokens, pre_gain, input_weight, output_weight, position_bias, post_gain):
    mp_size, dp_size = lax.axis_size("mp"), lax.axis_size("dp")
    seq_len, width = tokens.shape
    features = width * mp_size
    token_parts = from_shifts(tokens, mp_size)
    weight_parts = from_flips(input_weight, dp_size)
    gain_parts = [gain[None, :] for gain in from_shifts(pre_gain, mp_size)]
    params = pltpu.CompilerParams(vmem_limit_bytes=48 * 1024 * 1024)
    weights, own_tokens, bias = pl.pallas_call(
        lambda *refs: prepare_kernel(mp_size, dp_size, *refs),
        out_shape=(
            jax.ShapeDtypeStruct((features, 3 * width), jnp.bfloat16),
            jax.ShapeDtypeStruct(tokens.shape, tokens.dtype),
            jax.ShapeDtypeStruct(position_bias.shape, position_bias.dtype),
        ),
        in_specs=vmem_specs(dp_size + 2),
        out_specs=tuple(vmem_specs(3)),
        compiler_params=params,
        name="prepare",
    )(*weight_parts, tokens, position_bias)
    token_parts[0] = own_tokens
    token_parts, output_weight = lax.optimization_barrier((token_parts, output_weight))
    output_parts = from_shifts(output_weight, mp_size)
    context = pl.pallas_call(
        lambda *refs: attend_kernel(mp_size, *refs),
        out_shape=jax.ShapeDtypeStruct((seq_len, width), jnp.bfloat16),
        in_specs=vmem_specs(2 * mp_size + 2),
        out_specs=pl.BlockSpec(memory_space=pltpu.VMEM),
        scratch_shapes=[pltpu.VMEM((seq_len, features), jnp.bfloat16)],
        compiler_params=params,
        cost_estimate=pl.CostEstimate(
            flops=8 * 10**9, bytes_accessed=6 * 10**6, transcendentals=10**6
        ),
        name="attend",
    )(*token_parts, *gain_parts, weights, bias)
    context, output_parts = lax.optimization_barrier((context, output_parts))
    context_parts = from_shifts(context, mp_size)
    output_all = from_flips(jnp.stack(output_parts), dp_size)
    whole = jax.ShapeDtypeStruct((seq_len, width), jnp.bfloat16)
    columns = output_weight.shape[1]
    return tuple(
        pl.pallas_call(
            lambda *refs: finish_kernel(mp_size, dp_size, *refs),
            out_shape=(whole, whole),
            in_specs=vmem_specs(2 * mp_size + dp_size + 1),
            out_specs=tuple(vmem_specs(2)),
            scratch_shapes=[pltpu.VMEM((features // columns, seq_len, columns), jnp.bfloat16)],
            compiler_params=params,
            name="finish",
        )(*context_parts, *token_parts, *output_all, post_gain[None, :])
    )


def direct_fits(mesh):
    dp_size, mp_size = mesh.shape["dp"], mesh.shape["mp"]
    return 2 <= dp_size <= 8 and dp_size & (dp_size - 1) == 0 and mp_size <= 4


def body(mesh):
    def chosen(*arrays):
        tokens, input_weight, output_weight, position_bias = arrays[0], *arrays[2:5]
        whole_sequence = tokens.shape[0] == position_bias.shape[1]
        lanes_fit = output_weight.shape[1] % lane_width == 0
        rows_fit = tokens.shape[1] % input_weight.shape[1] == 0
        same_width = output_weight.shape[0] == tokens.shape[1] == input_weight.shape[2]
        if direct_fits(mesh) and whole_sequence and lanes_fit and rows_fit and same_width:
            return on_device_direct(*arrays)
        return on_device(*arrays)

    return chosen


def solution(mesh):
    return jax.shard_map(
        body(mesh),
        mesh=mesh,
        in_specs=(
            P("dp", "mp"),
            P("mp"),
            P(None, "dp", "mp"),
            P("mp", "dp"),
            P("mp", None, None),
            P("mp"),
        ),
        out_specs=(P("dp", "mp"), P("dp", "mp")),
        check_vma=False,
    )
```
